128 devices in a mesh: dp: 16 (over y_hi, z, core), tensor: 8 (over y_lo, x).
Axes of the slice: x: 4, y: 4 (y_hi: 2, y_lo: 2; y = y_hi * 2 + y_lo), z: 4, core: 2. Of those that a mesh axis runs over, the one named last changes fastest.
Arguments:
- saved_queries: bfloat16 [16384, 8192], P('dp', 'tensor'), may hold values from -200 to 200
- saved_keys: bfloat16 [16384, 1024], P('dp', 'tensor'), may hold values from -200 to 200
- saved_values: bfloat16 [16384, 1024], P('dp', 'tensor'), may hold values from -6 to 6
- out_grad: bfloat16 [16384, 8192], P(('dp', 'tensor')), may hold values from -2.5 to 2.5
- act_exponent: int32 [1], replicated, may hold values from -6 to 3
- grad_exponent: int32 [1], replicated, may hold values from -4 to 1
Outputs:
- grad_weight: float32 [8192, 8192], P('dp', 'tensor')
The draws below stay inside these ranges and needn't reach their ends.
All inputs are finite; a program needn't handle non-finite values.
Results may differ from the reference program's by a relative error of at most 0.012.
Values may be sent and summed in bfloat16 or wider, within the bound.
A program may use at most 128 MiB of HBM per device.

```python
import jax
import jax.numpy as jnp
from jax import lax

D = 8192
HEADS = 64
KV_HEADS = 8
HEAD_DIM = 128
SEQ = 1024
TOKENS = 16384
N_DP = 16


def query_keys(key):
    base = jax.random.fold_in(key, 11)
    first, second = jax.random.split(base)
    queries = jnp.clip(jax.random.normal(first, (TOKENS, HEADS * HEAD_DIM), jnp.float32), -5.0, 5.0)
    keys_all = jnp.clip(jax.random.normal(second, (TOKENS, KV_HEADS * HEAD_DIM), jnp.float32), -5.0, 5.0)
    return (queries, keys_all)


def draw_saved_queries(key, part):
    return query_keys(key)[0].astype(jnp.bfloat16)


def draw_saved_keys(key, part):
    return query_keys(key)[1].astype(jnp.bfloat16)


def raised(entries, stream_key, source, target, parts, factor):
    def block_of(axis_at):
        return (jnp.arange(entries.shape[axis_at]) // (entries.shape[axis_at] // parts)).reshape((-1,) + (1,) * (entries.ndim - 1 - axis_at))

    near = jax.random.permutation(stream_key, parts)[block_of(target)]
    second = (block_of(target) + parts // 2) % parts
    return jnp.where((block_of(source) == near) | (block_of(source) == second), factor * entries, entries)


def steps_of(rng, extent, cuts, low, largest):
    factor_of = 1.0
    for dim, blocks in cuts:
        steps = jax.random.uniform(jax.random.fold_in(jax.random.fold_in(rng, 6), dim), (blocks,), jnp.float32, low / len(cuts), largest / len(cuts))
        factor_of = factor_of * jnp.repeat(jnp.exp(steps), extent[dim] // blocks).reshape((-1,) + (1,) * (len(extent) - 1 - dim))
    return factor_of


def centred(key, shape, deviation, reach, cuts=(), kind=jnp.bfloat16):
    array = jax.random.normal(key, shape, jnp.float32) * deviation
    if len(cuts) > 0:
        array = steps_of(key, shape, cuts, -0.22, 0.18) * array
    return jnp.clip(array, min=-reach, max=reach).astype(kind)


def heavy_noise(rng, shape, width, limit, shards, heavy, kind=jnp.bfloat16):
    drawn = width * jax.random.normal(rng, shape, jnp.float32)
    if shards:
        drawn = drawn * steps_of(rng, shape, shards, -0.22, 0.18)
    return jnp.clip(raised(drawn, jax.random.fold_in(rng, 3), *heavy), -limit, limit).astype(kind)


def setup_inputs(seed: int = 0) -> dict:
    splits = jax.random.split(jax.random.key(seed), 7)
    return {
        "saved_queries": draw_saved_queries(jax.random.fold_in(splits[6], 71), 0),
        "saved_keys": draw_saved_keys(jax.random.fold_in(splits[6], 71), 0),
        "saved_values": centred(splits[2], (TOKENS, KV_HEADS * HEAD_DIM), 1.0, 6.0, ((0, 16), (1, 8))),
        "out_grad": heavy_noise(splits[3], (TOKENS, D), 0.1, 2.5, ((0, 128),), (0, 1, 128, 5.5)),
        "act_exponent": jax.random.randint(splits[4], (1,), -6, 4).astype(jnp.int32),
        "grad_exponent": jax.random.randint(splits[5], (1,), -4, 2).astype(jnp.int32),
    }


SATURATION = 448.0

def quantize(values_in, exponent):
    factor = SATURATION * jnp.exp2(-exponent[0].astype(jnp.float32))
    return jnp.clip(values_in * factor, -SATURATION, SATURATION).astype(jnp.bfloat16)

def attend(query_rows, key_rows, value_rows):
    scores = jnp.dot(query_rows, key_rows.T, preferred_element_type=jnp.float32) * HEAD_DIM ** (-0.5)
    positions = jnp.arange(query_rows.shape[0], dtype=jnp.int32)
    causal = positions[None, :] <= positions[:, None]
    scores = jnp.where(causal, scores, jnp.float32(-1e+30))
    row_max = lax.optimization_barrier(jnp.max(scores, axis=1, keepdims=True))
    weights = jnp.exp(scores - row_max)
    probabilities = (weights / lax.optimization_barrier(jnp.sum(weights, axis=1, keepdims=True))).astype(jnp.bfloat16)
    return jnp.dot(probabilities, value_rows, preferred_element_type=jnp.float32)

def reference(saved_queries, saved_keys, saved_values, out_grad, act_exponent, grad_exponent):
    per_group = HEADS // KV_HEADS
    dequant = jnp.exp2((act_exponent[0] + grad_exponent[0]).astype(jnp.float32)) / (SATURATION * SATURATION)

    def sequence_grad(running, seq_index):
        offset = (seq_index * SEQ).astype(jnp.int32)
        seq_queries = lax.dynamic_slice_in_dim(saved_queries, offset, SEQ, 0)
        seq_keys = lax.dynamic_slice_in_dim(saved_keys, offset, SEQ, 0)
        seq_values = lax.dynamic_slice_in_dim(saved_values, offset, SEQ, 0)
        seq_grad = lax.dynamic_slice_in_dim(out_grad, offset, SEQ, 0)

        def one_head(head_index):
            query_rows = lax.dynamic_slice_in_dim(seq_queries, (head_index * HEAD_DIM).astype(jnp.int32), HEAD_DIM, 1)
            kv_start = (head_index // per_group * HEAD_DIM).astype(jnp.int32)
            key_rows = lax.dynamic_slice_in_dim(seq_keys, kv_start, HEAD_DIM, 1)
            value_rows = lax.dynamic_slice_in_dim(seq_values, kv_start, HEAD_DIM, 1)
            return attend(query_rows, key_rows, value_rows)
        attended = lax.map(one_head, jnp.arange(HEADS, dtype=jnp.int32))
        attended = jnp.transpose(attended, (1, 0, 2)).reshape(SEQ, HEADS * HEAD_DIM)
        act_scaled = quantize(attended, act_exponent)
        grad_scaled = quantize(seq_grad.astype(jnp.float32), grad_exponent)
        seq_partial = lax.dot_general(grad_scaled, act_scaled, (((0,), (0,)), ((), ())), preferred_element_type=jnp.float32)
        seq_partial = (seq_partial * dequant).astype(jnp.bfloat16)
        return (running + seq_partial.astype(jnp.float32), None)
    zero_sum = jnp.zeros((D, HEADS * HEAD_DIM), jnp.float32)
    grad_weight, unused = lax.scan(sequence_grad, zero_sum, jnp.arange(N_DP, dtype=jnp.int32))
    return grad_weight
```

```python
import math

import jax
import jax.numpy as jnp
from jax import lax
from jax.experimental import pallas as pl
from jax.experimental.pallas import tpu as pltpu
from jax.sharding import PartitionSpec as P

MESH = pl.DeviceIdType.MESH
SATURATION = 448.0
HEAD_DIM = 128
EXPONENT_SCALE = HEAD_DIM**-0.5 * math.log2(math.e)
BF16, F32 = jnp.bfloat16, jnp.float32
VMEM_LIMIT = 67_043_328

OWN = 0
OTHER = 1


def schedule():
    steps = [("mm", 0, OWN, 0), ("mm", 0, OWN, 1)]
    for o in range(1, 8):
        steps.append(("ring", o + 1))
        steps += [("mm", o, OWN, 0), ("mm", o, OWN, 1)]
        if o == 3:
            steps.append(("attended", 0))
        if o == 4:
            steps += [("mm", k, OTHER, 0) for k in range(5)]
        if o in (5, 6):
            steps.append(("mm", o, OTHER, 0))
        if o == 6:
            steps.append(("attended", 1))
            steps += [("mm", k, OTHER, 1) for k in range(7)]
    steps += [("mm", 7, OTHER, 0), ("mm", 7, OTHER, 1)]
    return steps


def kernel(q_hbm, k_hbm, v_hbm, g_hbm, ae_ref, ge_ref, out_ref,
           q_ref, k_ref, v_ref, g_in, vt_ref, g_send, g_all, at_own, at_oth,
           z2_send, z2_recv, zf_send, zf_recv, y_send, y_recv, kept,
           in_sem, s1_send, s1_recv, x_send, x_recv, xf_send, xf_recv, a_send, a_recv,
           z2_ssem, z2_rsem, zf_ssem, zf_rsem, y_ssem, y_rsem):
    d = lax.axis_index("dp")
    t = lax.axis_index("tensor")
    yh, z, c = lax.div(d, 8), lax.rem(lax.div(d, 2), 4), lax.rem(d, 2)
    low, x = lax.div(t, 4), lax.rem(t, 4)
    partner_dp = d + 1 - 2 * c
    side_t = (1 - low) * 4 + x
    far_dp = (1 - yh) * 8 + z * 2 + c
    x_up, x_down = lax.rem(x + 1, 4), lax.rem(x + 3, 4)
    z_up, z_down = lax.rem(z + 1, 4), lax.rem(z + 3, 4)

    def dev(dp, tensor):
        return {"dp": dp, "tensor": tensor}

    core_dev, side_dev, cross_dev = dev(partner_dp, t), dev(d, side_t), dev(partner_dp, side_t)
    xp_dev, xm_dev = dev(d, low * 4 + x_up), dev(d, low * 4 + x_down)
    zp_dev, zm_dev = dev(yh * 8 + z_up * 2 + c, t), dev(yh * 8 + z_down * 2 + c, t)
    far_dev, far_side_dev = dev(far_dp, t), dev(far_dp, side_t)
    quarter_dev = (core_dev, side_dev, cross_dev)
    quarter_slot = ((1 - c, low), (c, 1 - low), (1 - c, 1 - low))

    def remote(src, dst, ssem, rsem, to):
        return pltpu.make_async_remote_copy(
            src_ref=src, dst_ref=dst, send_sem=ssem, recv_sem=rsem, device_id=to, device_id_type=MESH
        )

    loads = [
        pltpu.make_async_copy(src, dst, in_sem.at[i])
        for i, (src, dst) in enumerate(((g_hbm, g_in), (k_hbm, k_ref), (v_hbm, v_ref), (q_hbm, q_ref)))
    ]
    for load in loads:
        load.start()
    barrier = pltpu.get_barrier_semaphore()
    for to in (core_dev, side_dev, cross_dev, xp_dev, xm_dev, zp_dev, zm_dev, far_dev, far_side_dev):
        pl.semaphore_signal(barrier, inc=1, device_id=to, device_id_type=MESH)

    grad_factor = SATURATION * jnp.exp2(jnp.full((1, 256), -ge_ref[0], jnp.int32).astype(F32))
    act_factor = SATURATION * jnp.exp2(jnp.full((1, 256), -ae_ref[0], jnp.int32).astype(F32))
    dequant = jnp.exp2(jnp.full((1, 256), ae_ref[0] + ge_ref[0], jnp.int32).astype(F32)) / (
        SATURATION * SATURATION
    )

    def block_of(o):
        role = lax.div(o, 2)
        shift = jnp.where(role == 0, 2, jnp.where(role == 1, 1, jnp.where(role == 2, 3, 0)))
        to_z = lax.rem(z + shift, 4)
        to_yh = jnp.where(lax.rem(o, 2) == 0, 1 - yh, yh)
        return to_yh * 16 + to_z * 4

    def s1_copy(k, o):
        return remote(g_send.at[k, o], g_all.at[o, c, low, x], s1_send.at[k, o], s1_recv.at[k, o], quarter_dev[k])

    def s1_wait(k, o):
        s, l = quarter_slot[k]
        remote(g_send.at[k, o], g_all.at[o, s, l, x], s1_send.at[k, o], s1_recv.at[k, o], quarter_dev[k]).wait_recv()

    loads[0].wait()

    def scaled(block):
        values = g_in[:, pl.ds(pl.multiple_of(block * 256, 256), 256)].astype(F32)
        return jnp.clip(values * grad_factor, -SATURATION, SATURATION).astype(BF16)

    def quantize_block(o, carry):
        base = block_of(o)
        g_send[1, o] = scaled(base + 2 * c + 1 - low)
        g_send[2, o] = scaled(base + 2 * (1 - c) + 1 - low)
        g_send[0, o] = scaled(base + 2 * (1 - c) + low)
        g_all[o, c, low, x] = scaled(base + 2 * c + low)
        return carry

    lax.fori_loop(0, 8, quantize_block, 0)
    pl.semaphore_wait(barrier, 9)

    def send_block(o, carry):
        for k in (1, 2, 0):
            s1_copy(k, o).start()
        return carry

    lax.fori_loop(0, 8, send_block, 0)

    def x_copy(o, i):
        src = g_all.at[o, :, :, x]
        return remote(src, src, x_send.at[i, o], x_recv.at[i, o], (xp_dev, xm_dev)[i])

    def x_arrival(o, i):
        src = g_all.at[o, :, :, (x_down, x_up)[i]]
        return remote(src, src, x_send.at[i, o], x_recv.at[i, o], (xp_dev, xm_dev)[i])

    def xf_copy(o, i):
        src = g_all.at[o, i, :, (x_down, x_up)[i]]
        return remote(src, src, xf_send.at[i, o], xf_recv.at[i, o], (xp_dev, xm_dev)[i])

    def xf_arrival(o, i):
        src = g_all.at[o, i, :, lax.rem(x + 2, 4)]
        return remote(src, src, xf_send.at[i, o], xf_recv.at[i, o], (xp_dev, xm_dev)[i])

    def ring_start(o):
        for k in range(3):
            s1_wait(k, o)
        for i in range(2):
            x_copy(o, i).start()

    def ring_forward(o):
        for i in range(2):
            x_arrival(o, i).wait_recv()
            xf_copy(o, i).start()

    def a_rows(half):
        return pl.ds(pl.multiple_of(half * 512, 512), 512)

    def a_copy(half, i):
        src = at_own.at[c, a_rows(half)]
        dst = at_own.at[c, a_rows(half)] if i == 0 else at_oth.at[c, a_rows(half)]
        return remote(src, dst, a_send.at[i, half], a_recv.at[i, half], (core_dev, side_dev)[i])

    def a_forward(half):
        src = at_oth.at[c, a_rows(half)]
        return remote(src, src, a_send.at[2, half], a_recv.at[2, half], core_dev)

    def a_wait(half, i):
        ref = at_own.at[1 - c, a_rows(half)] if i == 0 else at_oth.at[c if i == 1 else 1 - c, a_rows(half)]
        remote(ref, ref, a_send.at[i, half], a_recv.at[i, half], (core_dev, side_dev, core_dev)[i]).wait_recv()

    for load in loads[1:]:
        load.wait()
    vt_ref[...] = v_ref[...].astype(F32).T.astype(BF16)
    causal = lax.broadcasted_iota(jnp.int32, (256, 256), 0) <= lax.broadcasted_iota(jnp.int32, (256, 256), 1)

    def head(index):
        columns = pl.ds(pl.multiple_of(index * HEAD_DIM, HEAD_DIM), HEAD_DIM)
        for tb in range(4):
            rows = slice(tb * 256, (tb + 1) * 256)
            query = q_ref[rows, columns]

            def scores_of(keys):
                return lax.dot_general(keys, query, (((1,), (1,)), ((), ())), preferred_element_type=F32)

            last = jnp.where(causal, scores_of(k_ref[rows, :]), F32(-1e30))
            top = jnp.max(last, axis=0, keepdims=True)
            if tb > 0:
                early = scores_of(k_ref[: tb * 256, :])
                top = jnp.maximum(top, jnp.max(early, axis=0, keepdims=True))
            weights = jnp.exp2((last - top) * EXPONENT_SCALE)
            total = jnp.sum(weights, axis=0, keepdims=True)
            value = jnp.dot(vt_ref[:, rows], weights.astype(BF16), preferred_element_type=F32)
            if tb > 0:
                weights = jnp.exp2((early - top) * EXPONENT_SCALE)
                total += jnp.sum(weights, axis=0, keepdims=True)
                value += jnp.dot(vt_ref[:, : tb * 256], weights.astype(BF16), preferred_element_type=F32)
            value = jnp.clip(value * (act_factor / total), -SATURATION, SATURATION).astype(BF16)
            at_own[c, columns, rows] = value

    def two_heads(i, carry):
        head(2 * i)
        head(2 * i + 1)

        @pl.when(i >= 2)
        def _():
            ring_forward(i - 2)

        ring_start(i)

        @pl.when(lax.rem(i, 2) == 1)
        def _():
            half = lax.div(i, 2)
            a_copy(half, 0).start()
            a_copy(half, 1).start()

        return carry

    lax.fori_loop(0, 4, two_heads, 0)

    def z2_copy(stream, half):
        return remote(z2_send.at[stream, half], z2_recv.at[stream, half], z2_ssem.at[stream, half],
                      z2_rsem.at[stream, half], (zp_dev, zm_dev)[half])

    def zf_copy(way, stream, half):
        return remote(zf_send.at[way, stream, half], zf_recv.at[way, stream, half], zf_ssem.at[way, stream, half],
                      zf_rsem.at[way, stream, half], (zp_dev, zm_dev)[way])

    def y_copy(k, half):
        return remote(y_send.at[k, half], y_recv.at[k, half], y_ssem.at[k, half], y_rsem.at[k, half],
                      (far_dev, side_dev, far_side_dev)[k])

    have = set()

    def need(key, wait):
        if key not in have:
            have.add(key)
            wait()

    def multiply(o, which, half):
        for i in range(2):
            need(("x", o, i), lambda: x_arrival(o, i).wait_recv())
            need(("xf", o, i), lambda: xf_arrival(o, i).wait_recv())
        if which == OWN:
            need(("a0", half), lambda: a_wait(half, 0))
        else:
            need(("a2", half), lambda: a_wait(half, 2))
        role, far = o // 2, o % 2 == 0
        stream = 2 * (o % 2) + which
        adds, copy = [], None
        if role == 0:
            dst, copy = z2_send.at[stream, half], z2_copy(stream, half)
        elif role < 3:
            way = role - 1
            dst, copy = zf_send.at[way, stream, half], zf_copy(way, stream, half)
            if way == half:
                z2_copy(stream, half).wait_recv()
                adds = [z2_recv.at[stream, half]]
        else:
            for way in range(2):
                zf_copy(way, stream, half).wait_recv()
            adds = [zf_recv.at[way, stream, half] for way in range(2)]
            if which == OWN and not far:
                dst = kept.at[half]
            else:
                k = 0 if which == OWN else (2 if far else 1)
                dst, copy = y_send.at[k, half], y_copy(k, half)
        at = (at_own, at_oth)[which]

        def tile(n, carry):
            rows = pl.ds(pl.multiple_of(half * 512 + n * 256, 256), 256)
            part = pl.ds(pl.multiple_of(n * 256, 256), 256)
            total = jnp.dot(at[0, rows, :], g_all[o, 0].reshape(1024, 256), preferred_element_type=F32)
            total += jnp.dot(at[1, rows, :], g_all[o, 1].reshape(1024, 256), preferred_element_type=F32)
            for add in adds:
                total += add[part, :].astype(F32)
            dst[part, :] = total.astype(BF16)
            return carry

        lax.fori_loop(0, 2, tile, 0)
        if copy is not None:
            copy.start()

    ring_forwarded, ring_started = 2, 4
    for step in schedule():
        if step[0] == "ring":
            if ring_forwarded < 8:
                for i in range(2):
                    x_arrival(ring_forwarded, i).wait_recv()
                    xf_copy(ring_forwarded, i).start()
                ring_forwarded += 1
            if ring_started < 8:
                ring_start(ring_started)
                ring_started += 1
            have.update(("x", o, i) for o in range(ring_forwarded) for i in range(2))
        elif step[0] == "attended":
            a_wait(step[1], 1)
            a_forward(step[1]).start()
        else:
            have.update(("x", o, i) for o in range(2) for i in range(2))
            multiply(*step[1:])

    for half in range(2):
        rows = slice(half * 512, (half + 1) * 512)
        for k in range(3):
            y_copy(k, half).wait_recv()
        mine = kept[half].astype(F32) + y_recv[0, half].astype(F32)
        out_ref[rows, pl.ds(pl.multiple_of(low * 256, 256), 256)] = mine * dequant
        theirs = y_recv[1, half].astype(F32) + y_recv[2, half].astype(F32)
        out_ref[rows, pl.ds(pl.multiple_of((1 - low) * 256, 256), 256)] = theirs * dequant

    def drain(o, carry):
        for k in range(3):
            s1_copy(k, o).wait_send()
        for i in range(2):
            x_copy(o, i).wait_send()
            xf_copy(o, i).wait_send()
        return carry

    lax.fori_loop(0, 8, drain, 0)
    for half in range(2):
        a_copy(half, 0).wait_send()
        a_copy(half, 1).wait_send()
        a_forward(half).wait_send()
        for k in range(3):
            y_copy(k, half).wait_send()
        for stream in range(4):
            z2_copy(stream, half).wait_send()
            for way in range(2):
                zf_copy(way, stream, half).wait_send()


def on_device(queries, keys, values, out_grad, act_exponent, grad_exponent):
    anywhere = pl.BlockSpec(memory_space=pl.ANY)
    scalar = pl.BlockSpec(memory_space=pltpu.SMEM)
    dma = pltpu.SemaphoreType.DMA
    transposed = pl.pallas_call(
        kernel,
        name="project_grad",
        out_shape=jax.ShapeDtypeStruct((1024, 512), F32),
        in_specs=[anywhere] * 4 + [scalar] * 2,
        out_specs=pl.BlockSpec(memory_space=pltpu.VMEM),
        scratch_shapes=[
            pltpu.VMEM((1024, 1024), BF16),
            pltpu.VMEM((1024, 128), BF16),
            pltpu.VMEM((1024, 128), BF16),
            pltpu.VMEM((128, 8192), BF16),
            pltpu.VMEM((128, 1024), BF16),
            pltpu.VMEM((3, 8, 128, 256), BF16),
            pltpu.VMEM((8, 2, 2, 4, 128, 256), BF16),
            pltpu.VMEM((2, 1024, 1024), BF16),
            pltpu.VMEM((2, 1024, 1024), BF16),
            pltpu.VMEM((4, 2, 512, 256), BF16),
            pltpu.VMEM((4, 2, 512, 256), BF16),
            pltpu.VMEM((2, 4, 2, 512, 256), BF16),
            pltpu.VMEM((2, 4, 2, 512, 256), BF16),
            pltpu.VMEM((3, 2, 512, 256), BF16),
            pltpu.VMEM((3, 2, 512, 256), BF16),
            pltpu.VMEM((2, 512, 256), BF16),
            dma((4,)),
            dma((3, 8)), dma((3, 8)),
            dma((2, 8)), dma((2, 8)),
            dma((2, 8)), dma((2, 8)),
            dma((3, 2)), dma((3, 2)),
            dma((4, 2)), dma((4, 2)),
            dma((2, 4, 2)), dma((2, 4, 2)),
            dma((3, 2)), dma((3, 2)),
        ],
        compiler_params=pltpu.CompilerParams(
            collective_id=0, has_side_effects=True, vmem_limit_bytes=VMEM_LIMIT
        ),
    )(queries, keys, values, out_grad, act_exponent, grad_exponent)
    return transposed.T


def solution(mesh):
    in_specs = (
        P("dp", "tensor"),
        P("dp", "tensor"),
        P("dp", "tensor"),
        P(("dp", "tensor"), None),
        P(),
        P(),
    )
    return jax.shard_map(
        on_device, mesh=mesh, in_specs=in_specs, out_specs=P("dp", "tensor"), check_vma=False
    )
```

```python
import math

import jax
import jax.numpy as jnp
from jax import lax
from jax.experimental import pallas as pl
from jax.experimental.pallas import tpu as pltpu
from jax.sharding import PartitionSpec as P

MESH = pl.DeviceIdType.MESH
SATURATION = 448.0
HEAD_DIM = 128
EXPONENT_SCALE = HEAD_DIM**-0.5 * math.log2(math.e)
BF16, F32 = jnp.bfloat16, jnp.float32
VMEM_LIMIT = 67_043_328
OWN, OTHER = 0, 1

STEPS = (
    ("rows", 0), ("rows", 1), ("rows", 2), ("head", 0), ("near", 0), ("head", 1), ("cols", 0), ("rows", 3),
    ("rows", 4), ("head", 2), ("side", 0), ("near", 1), ("head", 3), ("cols", 1), ("rows", 5), ("head", 4),
    ("head", 5), ("cols", 2), ("rows", 6), ("rows", 7), ("pass", 0), ("side", 1), ("near", 2), ("head", 6),
    ("head", 7), ("cols", 3), ("mm", 0, 0, 1), ("mm", 0, 0, 3), ("pass", 1), ("side", 2), ("near", 3),
    ("relay", 0), ("mm", 1, 0, 0), ("mm", 1, 0, 1), ("mm", 1, 0, 3), ("mm", 1, 0, 2), ("mm", 1, 1, 0), ("pass", 2),
    ("side", 3), ("near", 4), ("mm", 0, 1, 0), ("mm", 2, 0, 0), ("mm", 2, 0, 1), ("mm", 2, 0, 2), ("mm", 2, 0, 3),
    ("mm", 2, 1, 0), ("mm", 0, 0, 0), ("pass", 3), ("side", 4), ("near", 5), ("relay", 1), ("mm", 0, 1, 1),
    ("mm", 3, 0, 0), ("mm", 3, 0, 1), ("mm", 3, 0, 2), ("mm", 3, 0, 3), ("mm", 1, 1, 1), ("mm", 3, 1, 0),
    ("pass", 4), ("side", 5), ("near", 6), ("mm", 3, 1, 1), ("mm", 2, 1, 1), ("mm", 4, 0, 1), ("mm", 4, 0, 3),
    ("mm", 4, 1, 0), ("mm", 4, 1, 1), ("mm", 4, 0, 0), ("pass", 5), ("relay", 2), ("mm", 0, 1, 2), ("mm", 1, 1, 2),
    ("side", 6), ("near", 7), ("mm", 3, 1, 2), ("mm", 2, 1, 2), ("mm", 4, 1, 2), ("mm", 5, 0, 0), ("mm", 5, 0, 1),
    ("mm", 5, 0, 3), ("mm", 5, 1, 0), ("mm", 5, 1, 1), ("mm", 5, 1, 2), ("mm", 0, 0, 2), ("pass", 6), ("side", 7),
    ("mm", 4, 0, 2), ("mm", 6, 1, 1), ("mm", 6, 0, 1), ("mm", 6, 0, 3), ("mm", 6, 0, 0), ("mm", 6, 0, 2),
    ("mm", 6, 1, 0), ("mm", 6, 1, 2), ("pass", 7), ("relay", 3), ("mm", 0, 1, 3), ("mm", 1, 1, 3), ("mm", 2, 1, 3),
    ("mm", 5, 1, 3), ("mm", 7, 0, 1), ("mm", 7, 1, 1), ("mm", 7, 0, 3), ("mm", 4, 1, 3), ("mm", 3, 1, 3),
    ("mm", 7, 1, 0), ("mm", 5, 0, 2), ("mm", 7, 1, 2), ("mm", 6, 1, 3), ("mm", 7, 1, 3), ("mm", 7, 0, 0),
    ("mm", 7, 0, 2),
)
BLOCKS = ((0, 1), (0, 0), (2, 0), (1, 0), (1, 1), (2, 1), (3, 0), (3, 1))
EARLY = (0, 2)
WAY = ((0, 0, 1, 1), (0, 1, 1, 0))
SHIFT = (2, 1, 3, 0)


def kernel(q_hbm, k_hbm, v_hbm, g_hbm, ae_ref, ge_ref, out_ref,
           q_ref, k_ref, v_ref, g_in, vt_ref, g_send, g_all, at_own, at_oth,
           z2_send, z2_recv, zf_send, zf_recv, f_send, f_recv, p_send, p_recv, e_send, e_recv, s_send, s_recv,
           in_sem, s1_ssem, s1_rsem, x_ssem, x_rsem, xf_ssem, xf_rsem, a_ssem, a_rsem,
           z2_ssem, z2_rsem, zf_ssem, zf_rsem, f_ssem, f_rsem, l_ssem, l_rsem):
    d = lax.axis_index("dp")
    t = lax.axis_index("tensor")
    yh, z, c = lax.div(d, 8), lax.rem(lax.div(d, 2), 4), lax.rem(d, 2)
    low, x = lax.div(t, 4), lax.rem(t, 4)
    half = lax.rem(low + yh, 2)
    partner_dp = d + 1 - 2 * c
    side_t = (1 - low) * 4 + x
    x_up, x_down, x_far = lax.rem(x + 1, 4), lax.rem(x + 3, 4), lax.rem(x + 2, 4)
    z_up, z_down = lax.rem(z + 1, 4), lax.rem(z + 3, 4)

    def dev(dp, tensor):
        return {"dp": dp, "tensor": tensor}

    core_dev, side_dev, cross_dev = dev(partner_dp, t), dev(d, side_t), dev(partner_dp, side_t)
    x_devs = dev(d, low * 4 + x_up), dev(d, low * 4 + x_down)
    z_devs = dev(yh * 8 + z_up * 2 + c, t), dev(yh * 8 + z_down * 2 + c, t)
    far_dev = dev((1 - yh) * 8 + z * 2 + c, side_t)
    quarter_dev = (core_dev, side_dev, cross_dev)
    quarter_slot = ((1 - c, low), (c, 1 - low), (1 - c, 1 - low))

    sends = []

    def remote(src, dst, ssem, rsem, to):
        return pltpu.make_async_remote_copy(
            src_ref=src, dst_ref=dst, send_sem=ssem, recv_sem=rsem, device_id=to, device_id_type=MESH
        )

    def start(copy):
        copy.start()
        sends.append(copy)

    loads = [
        pltpu.make_async_copy(src, dst, in_sem.at[i])
        for i, (src, dst) in enumerate(((g_hbm, g_in), (k_hbm, k_ref), (v_hbm, v_ref), (q_hbm, q_ref)))
    ]
    for load in loads:
        load.start()
    barrier = pltpu.get_barrier_semaphore()
    for to in (core_dev, side_dev, cross_dev, *x_devs, *z_devs, far_dev):
        pl.semaphore_signal(barrier, inc=1, device_id=to, device_id_type=MESH)

    grad_factor = SATURATION * jnp.exp2(jnp.full((1, 256), -ge_ref[0], jnp.int32).astype(F32))
    act_factor = SATURATION * jnp.exp2(jnp.full((1, 256), -ae_ref[0], jnp.int32).astype(F32))
    dequant = jnp.exp2(jnp.full((1, 256), ae_ref[0] + ge_ref[0], jnp.int32).astype(F32)) / (
        SATURATION * SATURATION
    )

    loads[0].wait()

    def scaled(block):
        values = g_in[:, pl.ds(pl.multiple_of(block * 256, 256), 256)].astype(F32)
        return jnp.clip(values * grad_factor, -SATURATION, SATURATION).astype(BF16)

    for o, (role, near) in enumerate(BLOCKS):
        to_yh = yh if near else 1 - yh
        base = to_yh * 16 + lax.rem(z + SHIFT[role], 4) * 4
        g_send[1, o] = scaled(base + 2 * c + 1 - half)
        g_send[2, o] = scaled(base + 2 * (1 - c) + 1 - half)
        g_send[0, o] = scaled(base + 2 * (1 - c) + half)
        g_all[o, c, low, x] = scaled(base + 2 * c + half)
    pl.semaphore_wait(barrier, 8)

    def s1_send(k, o):
        start(remote(g_send.at[k, o], g_all.at[o, c, low, x], s1_ssem.at[k, o], s1_rsem.at[k, o], quarter_dev[k]))

    def s1_wait(k, o):
        s, l = quarter_slot[k]
        remote(g_send.at[k, o], g_all.at[o, s, l, x], s1_ssem.at[k, o], s1_rsem.at[k, o], quarter_dev[k]).wait_recv()

    def x_copy(o, i, part, at):
        ref = g_all.at[o, :, 1 - low if part else low, at]
        return remote(ref, ref, x_ssem.at[i, part, o], x_rsem.at[i, part, o], x_devs[i])

    def xf_copy(o, i, at):
        ref = g_all.at[o, i, :, at]
        return remote(ref, ref, xf_ssem.at[i, o], xf_rsem.at[i, o], x_devs[i])

    def a_copy(i, q):
        rows = pl.ds(q * 256, 256)
        src = (at_oth if i == 2 else at_own).at[c, rows]
        dst = (at_own if i == 0 else at_oth).at[c, rows]
        return remote(src, dst, a_ssem.at[i, q], a_rsem.at[i, q], (core_dev, side_dev, core_dev)[i])

    def a_wait(i, q):
        rows = pl.ds(q * 256, 256)
        ref = (at_own if i == 0 else at_oth).at[c if i == 1 else 1 - c, rows]
        remote(ref, ref, a_ssem.at[i, q], a_rsem.at[i, q], (core_dev, side_dev, core_dev)[i]).wait_recv()

    have = set()

    def need(key, wait):
        if key not in have:
            have.add(key)
            wait()

    def need_x(o, i, part):
        need(("x", o, i, part), lambda: x_copy(o, i, part, (x_down, x_up)[i]).wait_recv())

    def head(index):
        columns = slice(index * HEAD_DIM, (index + 1) * HEAD_DIM)
        for tb in range(4):
            rows = slice(tb * 256, (tb + 1) * 256)
            query = q_ref[rows, columns]

            def scores_of(keys):
                return lax.dot_general(keys, query, (((1,), (1,)), ((), ())), preferred_element_type=F32)

            last = jnp.where(causal, scores_of(k_ref[rows, :]), F32(-1e30))
            top = jnp.max(last, axis=0, keepdims=True)
            if tb > 0:
                early = scores_of(k_ref[: tb * 256, :])
                top = jnp.maximum(top, jnp.max(early, axis=0, keepdims=True))
            weights = jnp.exp2((last - top) * EXPONENT_SCALE)
            total = jnp.sum(weights, axis=0, keepdims=True)
            value = jnp.dot(vt_ref[:, rows], weights.astype(BF16), preferred_element_type=F32)
            if tb > 0:
                weights = jnp.exp2((early - top) * EXPONENT_SCALE)
                total += jnp.sum(weights, axis=0, keepdims=True)
                value += jnp.dot(vt_ref[:, : tb * 256], weights.astype(BF16), preferred_element_type=F32)
            value = jnp.clip(value * (act_factor / total), -SATURATION, SATURATION).astype(BF16)
            at_own[c, columns, rows] = value

    def z2_copy(stream, which, q):
        way = WAY[which][q]
        return remote(z2_send.at[stream, q], z2_recv.at[stream, q], z2_ssem.at[stream, q], z2_rsem.at[stream, q],
                      z_devs[way])

    def zf_copy(way, stream, q):
        return remote(zf_send.at[way, stream, q], zf_recv.at[way, stream, q], zf_ssem.at[way, stream, q],
                      zf_rsem.at[way, stream, q], z_devs[way])

    def f_copy(role, to_which, q):
        at = role, to_which, EARLY.index(q)
        return remote(f_send.at[at], f_recv.at[at], f_ssem.at[at], f_rsem.at[at], far_dev)

    def last_copy(i, q):
        send, recv = (p_send, e_send, s_send)[i], (p_recv, e_recv, s_recv)[i]
        return remote(send.at[q], recv.at[q], l_ssem.at[i, q], l_rsem.at[i, q], (far_dev, far_dev, side_dev)[i])

    def multiply(o, which, q):
        role, near = BLOCKS[o]
        stream = 2 * near + which
        early = q in EARLY
        for part in range(2):
            need(("s1", o, part), None)
            for i in range(2):
                need_x(o, i, part)
        for i in range(2):
            need(("xf", o, i), lambda: xf_copy(o, i, x_far).wait_recv())
        if which == OWN:
            need(("a0", q), lambda: a_wait(0, q))
        else:
            need(("a1", q), None)
            need(("a2", q), lambda: a_wait(2, q))
        adds, copy, dst = [], None, None
        if early and not near:
            copy = f_copy(role, 1 - which, q)
            dst = f_send.at[role, 1 - which, EARLY.index(q)]
        else:
            if early:
                f_copy(role, which, q).wait_recv()
                adds.append(f_recv.at[role, which, EARLY.index(q)])
            if role == 0:
                dst, copy = z2_send.at[stream, q], z2_copy(stream, which, q)
            elif role < 3:
                way = role - 1
                dst, copy = zf_send.at[way, stream, q], zf_copy(way, stream, q)
                if way == WAY[which][q]:
                    z2_copy(stream, which, q).wait_recv()
                    adds.append(z2_recv.at[stream, q])
            else:
                for way in range(2):
                    zf_copy(way, stream, q).wait_recv()
                    adds.append(zf_recv.at[way, stream, q])
                if not near:
                    dst, copy = ((p_send, e_send)[which].at[q], last_copy(which, q))
                elif which == OTHER:
                    dst, copy = s_send.at[q], last_copy(2, q)
                    if not early:
                        last_copy(0, q).wait_recv()
                        adds.append(p_recv.at[q])
        at = (at_own, at_oth)[which]
        rows = slice(q * 256, (q + 1) * 256)
        total = jnp.dot(at[0, rows, :], g_all[o, 0].reshape(1024, 256), preferred_element_type=F32)
        total += jnp.dot(at[1, rows, :], g_all[o, 1].reshape(1024, 256), preferred_element_type=F32)
        for add in adds:
            total += add[...].astype(F32)
        if copy is None:
            out_ref[rows, pl.ds(pl.multiple_of(half * 256, 256), 256)] = total * dequant
        else:
            dst[...] = total.astype(BF16)
            start(copy)

    for o in range(8):
        s1_send(0, o)
    causal = None
    for step in STEPS:
        kind, at = step[0], step[1]
        if kind == "rows":
            s1_send(1, at)
            s1_send(2, at)
        elif kind == "near":
            s1_wait(0, at)
            have.add(("s1", at, 0))
            for i in range(2):
                start(x_copy(at, i, 0, x))
        elif kind == "side":
            s1_wait(1, at)
            s1_wait(2, at)
            have.add(("s1", at, 1))
            for i in range(2):
                start(x_copy(at, i, 1, x))
        elif kind == "pass":
            for i in range(2):
                need_x(at, i, 0)
                need_x(at, i, 1)
                start(xf_copy(at, i, (x_down, x_up)[i]))
        elif kind == "head":
            if at == 0:
                for load in loads[1:]:
                    load.wait()
                vt_ref[...] = v_ref[...].astype(F32).T.astype(BF16)
                causal = lax.broadcasted_iota(jnp.int32, (256, 256), 0) <= lax.broadcasted_iota(
                    jnp.int32, (256, 256), 1
                )
            head(at)
        elif kind == "cols":
            start(a_copy(0, at))
            start(a_copy(1, at))
        elif kind == "relay":
            a_wait(1, at)
            have.add(("a1", at))
            start(a_copy(2, at))
        else:
            multiply(*step[1:])

    for q in range(4):
        rows = slice(q * 256, (q + 1) * 256)
        if q not in EARLY:
            last_copy(1, q).wait_recv()
            out_ref[rows, pl.ds(pl.multiple_of(half * 256, 256), 256)] += e_recv[q].astype(F32) * dequant
    for q in range(4):
        rows = slice(q * 256, (q + 1) * 256)
        last_copy(2, q).wait_recv()
        out_ref[rows, pl.ds(pl.multiple_of((1 - half) * 256, 256), 256)] = s_recv[q].astype(F32) * dequant
    for copy in sends:
        copy.wait_send()


def on_device(queries, keys, values, out_grad, act_exponent, grad_exponent):
    anywhere = pl.BlockSpec(memory_space=pl.ANY)
    scalar = pl.BlockSpec(memory_space=pltpu.SMEM)
    dma = pltpu.SemaphoreType.DMA
    early = max(len(EARLY), 1)
    tile = (256, 256)
    transposed = pl.pallas_call(
        kernel,
        name="project_grad",
        out_shape=jax.ShapeDtypeStruct((1024, 512), F32),
        in_specs=[anywhere] * 4 + [scalar] * 2,
        out_specs=pl.BlockSpec(memory_space=pltpu.VMEM),
        scratch_shapes=[
            pltpu.VMEM((1024, 1024), BF16),
            pltpu.VMEM((1024, 128), BF16),
            pltpu.VMEM((1024, 128), BF16),
            pltpu.VMEM((128, 8192), BF16),
            pltpu.VMEM((128, 1024), BF16),
            pltpu.VMEM((3, 8, 128, 256), BF16),
            pltpu.VMEM((8, 2, 2, 4, 128, 256), BF16),
            pltpu.VMEM((2, 1024, 1024), BF16),
            pltpu.VMEM((2, 1024, 1024), BF16),
            pltpu.VMEM((4, 4, *tile), BF16), pltpu.VMEM((4, 4, *tile), BF16),
            pltpu.VMEM((2, 4, 4, *tile), BF16), pltpu.VMEM((2, 4, 4, *tile), BF16),
            pltpu.VMEM((4, 2, early, *tile), BF16), pltpu.VMEM((4, 2, early, *tile), BF16),
            pltpu.VMEM((4, *tile), BF16), pltpu.VMEM((4, *tile), BF16),
            pltpu.VMEM((4, *tile), BF16), pltpu.VMEM((4, *tile), BF16),
            pltpu.VMEM((4, *tile), BF16), pltpu.VMEM((4, *tile), BF16),
            dma((4,)),
            dma((3, 8)), dma((3, 8)),
            dma((2, 2, 8)), dma((2, 2, 8)),
            dma((2, 8)), dma((2, 8)),
            dma((3, 4)), dma((3, 4)),
            dma((4, 4)), dma((4, 4)),
            dma((2, 4, 4)), dma((2, 4, 4)),
            dma((4, 2, early)), dma((4, 2, early)),
            dma((3, 4)), dma((3, 4)),
        ],
        compiler_params=pltpu.CompilerParams(
            collective_id=0, has_side_effects=True, vmem_limit_bytes=VMEM_LIMIT
        ),
    )(queries, keys, values, out_grad, act_exponent, grad_exponent)
    return transposed.T


def solution(mesh):
    in_specs = (
        P("dp", "tensor"),
        P("dp", "tensor"),
        P("dp", "tensor"),
        P(("dp", "tensor"), None),
        P(),
        P(),
    )
    return jax.shard_map(
        on_device, mesh=mesh, in_specs=in_specs, out_specs=P("dp", "tensor"), check_vma=False
    )
```

```python
import math

import jax
import jax.numpy as jnp
from jax import lax
from jax.experimental import pallas as pl
from jax.experimental.pallas import tpu as pltpu
from jax.sharding import PartitionSpec as P

MESH = pl.DeviceIdType.MESH
SATURATION = 448.0
HEAD_DIM = 128
EXPONENT_SCALE = HEAD_DIM**-0.5 * math.log2(math.e)
BF16, F32 = jnp.bfloat16, jnp.float32
VMEM_LIMIT = 67_043_328
OWN, OTHER = 0, 1

STEPS = (
    ("rows", 0), ("rows", 1), ("rows", 2), ("self", 0), ("self", 1), ("head", 0), ("near", 0), ("head", 1),
    ("cols", 0), ("rows", 3), ("rows", 4), ("rows", 5), ("head", 2), ("head", 3), ("cols", 1), ("side", 0),
    ("near", 1), ("head", 4), ("head", 5), ("cols", 2), ("rows", 6), ("rows", 7), ("head", 6), ("pass", 0),
    ("side", 1), ("self", 2), ("near", 2), ("head", 7), ("cols", 3), ("mm", 0, 0, 1), ("mm", 0, 0, 0), ("pass", 1),
    ("side", 2), ("self", 3), ("near", 3), ("relay", 0), ("mm", 1, 0, 1), ("pass", 2), ("side", 3), ("self", 4),
    ("near", 4), ("mm", 2, 0, 1), ("mm", 2, 0, 0), ("pass", 3), ("side", 4), ("self", 5), ("near", 5),
    ("mm", 3, 0, 1), ("relay", 1), ("pass", 4), ("side", 5), ("self", 6), ("near", 6), ("mm", 2, 1, 0),
    ("mm", 1, 1, 0), ("mm", 3, 1, 0), ("mm", 0, 1, 0), ("mm", 4, 0, 1), ("mm", 4, 0, 0), ("mm", 4, 1, 0),
    ("pass", 5), ("relay", 2), ("mm", 3, 0, 0), ("mm", 4, 1, 1), ("mm", 0, 1, 1), ("side", 6), ("self", 7),
    ("near", 7), ("mm", 1, 1, 1), ("mm", 5, 0, 1), ("mm", 5, 1, 1), ("mm", 1, 0, 0), ("pass", 6), ("side", 7),
    ("mm", 2, 1, 1), ("mm", 5, 1, 0), ("mm", 3, 1, 1), ("mm", 6, 0, 0), ("mm", 6, 0, 1), ("mm", 6, 1, 0),
    ("pass", 7), ("relay", 3), ("mm", 6, 1, 1), ("mm", 0, 1, 2), ("mm", 1, 1, 2), ("mm", 4, 1, 2), ("mm", 5, 1, 2),
    ("mm", 7, 0, 1), ("mm", 5, 0, 0), ("mm", 2, 1, 2), ("mm", 7, 1, 1), ("mm", 3, 1, 2), ("mm", 7, 1, 0),
    ("mm", 6, 1, 2), ("mm", 7, 1, 2), ("mm", 7, 0, 0),
)
BLOCKS = ((0, 0), (0, 1), (1, 0), (1, 1), (2, 0), (2, 1), (3, 0), (3, 1))
EARLY = (0, 1)
WAY = ((1, 0), (1, 0, 0))
SHIFT = (2, 1, 3, 0)
GROUPS = ((0, 1), (2, 3)), ((0, 1), (2,), (3,))


def kernel(q_hbm, k_hbm, v_hbm, g_hbm, ae_ref, ge_ref, out_ref,
           q_ref, k_ref, v_ref, g_in, vt_ref, g_send, g_all, at_own, at_oth,
           z2_send, z2_recv, zf_send, zf_recv, f_send, f_recv, p_send, p_recv, e_send, e_recv, s_send, s_recv, out_v,
           in_sem, s1_ssem, s1_rsem, x_ssem, x_rsem, xf_ssem, xf_rsem, a_ssem, a_rsem,
           z2_ssem, z2_rsem, zf_ssem, zf_rsem, f_ssem, f_rsem, l_ssem, l_rsem, out_sem):
    d = lax.axis_index("dp")
    t = lax.axis_index("tensor")
    yh, z, c = lax.div(d, 8), lax.rem(lax.div(d, 2), 4), lax.rem(d, 2)
    low, x = lax.div(t, 4), lax.rem(t, 4)
    half = lax.rem(low + yh, 2)
    partner_dp = d + 1 - 2 * c
    side_t = (1 - low) * 4 + x
    x_up, x_down, x_far = lax.rem(x + 1, 4), lax.rem(x + 3, 4), lax.rem(x + 2, 4)
    z_up, z_down = lax.rem(z + 1, 4), lax.rem(z + 3, 4)

    def dev(dp, tensor):
        return {"dp": dp, "tensor": tensor}

    core_dev, side_dev, cross_dev = dev(partner_dp, t), dev(d, side_t), dev(partner_dp, side_t)
    x_devs = dev(d, low * 4 + x_up), dev(d, low * 4 + x_down)
    z_devs = dev(yh * 8 + z_up * 2 + c, t), dev(yh * 8 + z_down * 2 + c, t)
    far_dev = dev((1 - yh) * 8 + z * 2 + c, side_t)
    quarter_dev = (core_dev, side_dev, cross_dev)
    quarter_slot = ((1 - c, low), (c, 1 - low), (1 - c, 1 - low))

    def remote(src, dst, ssem, rsem, to):
        return pltpu.make_async_remote_copy(
            src_ref=src, dst_ref=dst, send_sem=ssem, recv_sem=rsem, device_id=to, device_id_type=MESH
        )

    def start(make, *key):
        make(*key).start()

    def sent(ref, ssem):
        remote(ref, ref, ssem, in_sem.at[0], core_dev).wait_send()

    loads = [
        pltpu.make_async_copy(src, dst, in_sem.at[i])
        for i, (src, dst) in enumerate(((g_hbm, g_in), (k_hbm, k_ref), (v_hbm, v_ref), (q_hbm, q_ref)))
    ]
    for load in loads:
        load.start()
    barrier = pltpu.get_barrier_semaphore()
    for to in (core_dev, side_dev, cross_dev, *x_devs, *z_devs, far_dev):
        pl.semaphore_signal(barrier, inc=1, device_id=to, device_id_type=MESH)

    grad_factor = SATURATION * jnp.exp2(jnp.full((1, 256), -ge_ref[0], jnp.int32).astype(F32))
    act_factor = SATURATION * jnp.exp2(jnp.full((1, 256), -ae_ref[0], jnp.int32).astype(F32))
    dequant = jnp.exp2(jnp.full((1, 256), ae_ref[0] + ge_ref[0], jnp.int32).astype(F32)) / (
        SATURATION * SATURATION
    )

    loads[0].wait()

    def scaled(block):
        values = g_in[:, pl.ds(pl.multiple_of(block * 256, 256), 256)].astype(F32)
        return jnp.clip(values * grad_factor, -SATURATION, SATURATION).astype(BF16)

    for o, (role, near) in enumerate(BLOCKS):
        to_yh = yh if near else 1 - yh
        base = to_yh * 16 + lax.rem(z + SHIFT[role], 4) * 4
        g_send[1, o] = scaled(base + 2 * c + 1 - half)
        g_send[2, o] = scaled(base + 2 * (1 - c) + 1 - half)
        g_send[0, o] = scaled(base + 2 * (1 - c) + half)
        g_all[o, c, low, x] = scaled(base + 2 * c + half)
    pl.semaphore_wait(barrier, 8)

    def s1_copy(k, o):
        return remote(g_send.at[k, o], g_all.at[o, c, low, x], s1_ssem.at[0], s1_rsem.at[k, o], quarter_dev[k])

    def s1_wait(k, o):
        s, l = quarter_slot[k]
        remote(g_send.at[k, o], g_all.at[o, s, l, x], s1_ssem.at[0], s1_rsem.at[k, o], quarter_dev[k]).wait_recv()

    def x_copy(o, i, part, at):
        if part == 2:
            ref = g_all.at[o, :, 1 - low, at]
        else:
            ref = g_all.at[o, 1 - c if part else c, low, at]
        return remote(ref, ref, x_ssem.at[i], x_rsem.at[i, o], x_devs[i])

    def xf_copy(o, i, at):
        ref = g_all.at[o, i, :, at]
        return remote(ref, ref, xf_ssem.at[i], xf_rsem.at[i, o], x_devs[i])

    def a_copy(i, q):
        rows = pl.ds(q * 256, 256)
        src = (at_oth if i == 2 else at_own).at[c, rows]
        dst = (at_own if i == 0 else at_oth).at[c, rows]
        return remote(src, dst, a_ssem.at[i], a_rsem.at[i, q], (core_dev, side_dev, core_dev)[i])

    def a_wait(i, q):
        rows = pl.ds(q * 256, 256)
        ref = (at_own if i == 0 else at_oth).at[c if i == 1 else 1 - c, rows]
        remote(ref, ref, a_ssem.at[i], a_rsem.at[i, q], (core_dev, side_dev, core_dev)[i]).wait_recv()

    have = set()

    def need(key, wait):
        if key not in have:
            have.add(key)
            wait()

    def need_x(o, i):
        ref = g_all.at[o, :, :, (x_down, x_up)[i]]
        need(("x", o, i), lambda: remote(ref, ref, x_ssem.at[i], x_rsem.at[i, o], x_devs[i]).wait_recv())

    def head(index):
        columns = slice(index * HEAD_DIM, (index + 1) * HEAD_DIM)
        for tb in range(4):
            rows = slice(tb * 256, (tb + 1) * 256)
            query = q_ref[rows, columns]

            def scores_of(keys):
                return lax.dot_general(keys, query, (((1,), (1,)), ((), ())), preferred_element_type=F32)

            last = jnp.where(causal, scores_of(k_ref[rows, :]), F32(-1e30))
            top = jnp.max(last, axis=0, keepdims=True)
            if tb > 0:
                early = scores_of(k_ref[: tb * 256, :])
                top = jnp.maximum(top, jnp.max(early, axis=0, keepdims=True))
            weights = jnp.exp2((last - top) * EXPONENT_SCALE)
            total = jnp.sum(weights, axis=0, keepdims=True)
            value = jnp.dot(vt_ref[:, rows], weights.astype(BF16), preferred_element_type=F32)
            if tb > 0:
                weights = jnp.exp2((early - top) * EXPONENT_SCALE)
                total += jnp.sum(weights, axis=0, keepdims=True)
                value += jnp.dot(vt_ref[:, : tb * 256], weights.astype(BF16), preferred_element_type=F32)
            value = jnp.clip(value * (act_factor / total), -SATURATION, SATURATION).astype(BF16)
            at_own[c, columns, rows] = value

    def z2_copy(stream, way, q):
        return remote(z2_send.at[stream, q], z2_recv.at[stream, q], z2_ssem.at[stream // 2], z2_rsem.at[stream, q],
                      z_devs[way])

    def zf_copy(way, stream, q):
        return remote(zf_send.at[way, stream, q], zf_recv.at[way, stream, q], zf_ssem.at[stream // 2],
                      zf_rsem.at[way, stream, q], z_devs[way])

    def f_copy(role, to_which, q):
        at = role, to_which, q - EARLY[0]
        return remote(f_send.at[at], f_recv.at[at], f_ssem.at[0], f_rsem.at[at], far_dev)

    def last_copy(i, q):
        send, recv = (p_send, e_send, s_send)[i], (p_recv, e_recv, s_recv)[i]
        return remote(send.at[q], recv.at[q], l_ssem.at[i], l_rsem.at[i, q], (far_dev, far_dev, side_dev)[i])

    def out_copy(part, q):
        side = 1 - half if part else half
        to = out_ref.at[pl.ds(q * 256, 256), pl.ds(pl.multiple_of(side * 256, 256), 256)]
        return pltpu.make_async_copy(out_v.at[part, q], to, out_sem.at[part, q])

    def multiply(o, which, group):
        role, near = BLOCKS[o]
        quarters = GROUPS[which][group]
        stream, way2 = 2 * near + which, WAY[which][group]
        early = quarters[0] in EARLY
        for part in range(3):
            need(("s1", o, part), None)
        for i in range(2):
            need_x(o, i)
            need(("xf", o, i), lambda: xf_copy(o, i, x_far).wait_recv())
        adds, make, key, send = [], None, (), None
        for q in quarters:
            need(("cols", q) if which == OWN else ("relay", q), None)
            need(("a", which, q), lambda: a_wait(2 * which, q))
        if early and not near:
            make, key, send = f_copy, (role, 1 - which), lambda q: f_send.at[role, 1 - which, q - EARLY[0]]
        else:
            if early:
                for q in quarters:
                    f_copy(role, which, q).wait_recv()
                adds.append(lambda q: f_recv.at[role, which, q - EARLY[0]])
            if role == 0:
                make, key, send = z2_copy, (stream, way2), lambda q: z2_send.at[stream, q]
            elif role < 3:
                make, key, send = zf_copy, (role - 1, stream), lambda q: zf_send.at[role - 1, stream, q]
                if role - 1 == way2:
                    for q in quarters:
                        z2_copy(stream, way2, q).wait_recv()
                    adds.append(lambda q: z2_recv.at[stream, q])
            else:
                for q in quarters:
                    for way in range(2):
                        zf_copy(way, stream, q).wait_recv()
                adds += [lambda q: zf_recv.at[0, stream, q], lambda q: zf_recv.at[1, stream, q]]
                if not near:
                    make, key, send = last_copy, (which,), lambda q: (p_send, e_send)[which].at[q]
                elif which == OTHER:
                    make, key, send = last_copy, (2,), lambda q: s_send.at[q]
                    if not early:
                        for q in quarters:
                            last_copy(0, q).wait_recv()
                        adds.append(lambda q: p_recv.at[q])
        at = (at_own, at_oth)[which]

        def tile(q):
            rows = pl.ds(q * 256 if isinstance(q, int) else pl.multiple_of(q * 256, 256), 256)
            total = jnp.dot(at[0, rows, :], g_all[o, 0].reshape(1024, 256), preferred_element_type=F32)
            total += jnp.dot(at[1, rows, :], g_all[o, 1].reshape(1024, 256), preferred_element_type=F32)
            for add in adds:
                total += add(q)[...].astype(F32)
            if make is None:
                out_v[0, q] = total * dequant
                if early:
                    out_copy(0, q).start()
            else:
                send(q)[...] = total.astype(BF16)
                make(*key, q).start()

        if len(quarters) == 1:
            tile(quarters[0])
        else:
            lax.fori_loop(0, len(quarters), lambda i, carry: (tile(quarters[0] + i), carry)[1], 0)

    for o in range(8):
        start(s1_copy, 0, o)
    causal = None
    for step in STEPS:
        kind, at = step[0], step[1]
        if kind == "rows":
            start(s1_copy, 1, at)
            start(s1_copy, 2, at)
        elif kind == "self":
            have.add(("s1", at, 0))
            for i in range(2):
                start(x_copy, at, i, 0, x)
        elif kind == "near":
            s1_wait(0, at)
            have.add(("s1", at, 1))
            for i in range(2):
                start(x_copy, at, i, 1, x)
        elif kind == "side":
            s1_wait(1, at)
            s1_wait(2, at)
            have.add(("s1", at, 2))
            for i in range(2):
                start(x_copy, at, i, 2, x)
        elif kind == "pass":
            for i in range(2):
                need_x(at, i)
                start(xf_copy, at, i, (x_down, x_up)[i])
        elif kind == "head":
            if at == 0:
                for load in loads[1:]:
                    load.wait()
                vt_ref[...] = v_ref[...].astype(F32).T.astype(BF16)
                causal = lax.broadcasted_iota(jnp.int32, (256, 256), 0) <= lax.broadcasted_iota(
                    jnp.int32, (256, 256), 1
                )
            head(at)
        elif kind == "cols":
            have.add(("cols", at))
            start(a_copy, 0, at)
            start(a_copy, 1, at)
        elif kind == "relay":
            a_wait(1, at)
            have.add(("relay", at))
            start(a_copy, 2, at)
        else:
            multiply(*step[1:])

    for q in range(4):
        if q not in EARLY:
            last_copy(1, q).wait_recv()
            out_v[0, q] += e_recv[q].astype(F32) * dequant
            out_copy(0, q).start()
    for q in range(4):
        last_copy(2, q).wait_recv()
        out_v[1, q] = s_recv[q].astype(F32) * dequant
        out_copy(1, q).start()
    late = slice(0, 4)
    if EARLY:
        late = slice(2, 4) if EARLY[0] == 0 else slice(0, 2)
        sent(f_send, f_ssem.at[0])
    sent(g_send, s1_ssem.at[0])
    for i in range(2):
        sent(g_all.at[:, :, :, x], x_ssem.at[i])
        sent(g_all.at[:, i, :, (x_down, x_up)[i]], xf_ssem.at[i])
        sent((p_send, e_send)[i].at[late], l_ssem.at[i])
    for i, ref in enumerate((at_own, at_own, at_oth)):
        sent(ref.at[c], a_ssem.at[i])
    sent(z2_send.at[2:4], z2_ssem.at[1])
    sent(z2_send.at[0:2, late], z2_ssem.at[0])
    sent(zf_send.at[:, 2:4], zf_ssem.at[1])
    sent(zf_send.at[:, 0:2, late], zf_ssem.at[0])
    sent(s_send, l_ssem.at[2])
    for q in range(4):
        for part in range(2):
            out_copy(part, q).wait()


def on_device(queries, keys, values, out_grad, act_exponent, grad_exponent):
    anywhere = pl.BlockSpec(memory_space=pl.ANY)
    scalar = pl.BlockSpec(memory_space=pltpu.SMEM)
    dma = pltpu.SemaphoreType.DMA
    early = max(len(EARLY), 1)
    tile = (256, 256)
    transposed = pl.pallas_call(
        kernel,
        name="project_grad",
        out_shape=jax.ShapeDtypeStruct((1024, 512), F32),
        in_specs=[anywhere] * 4 + [scalar] * 2,
        out_specs=anywhere,
        scratch_shapes=[
            pltpu.VMEM((1024, 1024), BF16),
            pltpu.VMEM((1024, 128), BF16),
            pltpu.VMEM((1024, 128), BF16),
            pltpu.VMEM((128, 8192), BF16),
            pltpu.VMEM((128, 1024), BF16),
            pltpu.VMEM((3, 8, 128, 256), BF16),
            pltpu.VMEM((8, 2, 2, 4, 128, 256), BF16),
            pltpu.VMEM((2, 1024, 1024), BF16),
            pltpu.VMEM((2, 1024, 1024), BF16),
            pltpu.VMEM((4, 4, *tile), BF16), pltpu.VMEM((4, 4, *tile), BF16),
            pltpu.VMEM((2, 4, 4, *tile), BF16), pltpu.VMEM((2, 4, 4, *tile), BF16),
            pltpu.VMEM((4, 2, early, *tile), BF16), pltpu.VMEM((4, 2, early, *tile), BF16),
            pltpu.VMEM((4, *tile), BF16), pltpu.VMEM((4, *tile), BF16),
            pltpu.VMEM((4, *tile), BF16), pltpu.VMEM((4, *tile), BF16),
            pltpu.VMEM((4, *tile), BF16), pltpu.VMEM((4, *tile), BF16),
            pltpu.VMEM((2, 4, *tile), F32),
            dma((4,)),
            dma((1,)), dma((3, 8)),
            dma((2,)), dma((2, 8)),
            dma((2,)), dma((2, 8)),
            dma((3,)), dma((3, 4)),
            dma((2,)), dma((4, 4)),
            dma((2,)), dma((2, 4, 4)),
            dma((1,)), dma((4, 2, early)),
            dma((3,)), dma((3, 4)),
            dma((2, 4)),
        ],
        compiler_params=pltpu.CompilerParams(
            collective_id=0, has_side_effects=True, vmem_limit_bytes=VMEM_LIMIT
        ),
    )(queries, keys, values, out_grad, act_exponent, grad_exponent)
    return transposed.T


def solution(mesh):
    in_specs = (
        P("dp", "tensor"),
        P("dp", "tensor"),
        P("dp", "tensor"),
        P(("dp", "tensor"), None),
        P(),
        P(),
    )
    return jax.shard_map(
        on_device, mesh=mesh, in_specs=in_specs, out_specs=P("dp", "tensor"), check_vma=False
    )
```

```python
import math

import jax
import jax.numpy as jnp
from jax import lax
from jax.experimental import pallas as pl
from jax.experimental.pallas import tpu as pltpu
from jax.sharding import PartitionSpec as P

MESH = pl.DeviceIdType.MESH
SATURATION = 448.0
HEAD_DIM = 128
EXPONENT_SCALE = HEAD_DIM**-0.5 * math.log2(math.e)
BF16, F32 = jnp.bfloat16, jnp.float32
VMEM_LIMIT = 67_043_328
OWN, OTHER = 0, 1

STEPS = (
    ("self", 0), ("rows", 2), ("rows", 3), ("rows", 0), ("self", 1), ("rows", 1), ("near", 0), ("near", 4),
    ("self", 3), ("head", 0), ("head", 1), ("cols", 0), ("near", 3), ("rows", 4), ("head", 2), ("head", 3),
    ("near", 1), ("head", 4), ("cols", 1), ("side", 3), ("rows", 5), ("head", 5), ("cols", 2), ("head", 6),
    ("self", 4), ("side", 0), ("rows", 6), ("side", 1), ("rows", 7), ("self", 2), ("pass", 0), ("pass", 3),
    ("head", 7), ("pass", 1), ("side", 4), ("relay", 0), ("side", 2), ("near", 2), ("mm", 0, 0, 0), ("cols", 3),
    ("mm", 3, 0, 1), ("pass", 4), ("mm", 0, 0, 1), ("mm", 1, 0, 1), ("mm", 1, 0, 0), ("pass", 2), ("relay", 1),
    ("near", 5), ("near", 7), ("side", 5), ("mm", 3, 1, 0), ("mm", 0, 1, 0), ("mm", 4, 0, 1), ("mm", 2, 0, 1),
    ("mm", 1, 1, 0), ("mm", 2, 0, 0), ("self", 5), ("near", 6), ("mm", 4, 1, 0), ("self", 6), ("relay", 2),
    ("pass", 5), ("mm", 3, 0, 0), ("mm", 3, 1, 1), ("side", 6), ("mm", 0, 1, 1), ("mm", 2, 1, 0), ("mm", 2, 1, 1),
    ("side", 7), ("mm", 5, 1, 1), ("mm", 4, 0, 0), ("pass", 6), ("mm", 5, 1, 0), ("mm", 4, 1, 1), ("mm", 5, 0, 1),
    ("self", 7), ("mm", 1, 1, 1), ("mm", 6, 0, 0), ("relay", 3), ("mm", 6, 0, 1), ("pass", 7), ("mm", 6, 1, 0),
    ("mm", 0, 1, 2), ("mm", 2, 1, 2), ("mm", 3, 1, 2), ("mm", 5, 1, 2), ("mm", 5, 0, 0), ("mm", 7, 1, 0),
    ("mm", 1, 1, 2), ("mm", 7, 0, 1), ("mm", 4, 1, 2), ("mm", 7, 1, 1), ("mm", 6, 1, 1), ("mm", 6, 1, 2),
    ("mm", 7, 1, 2), ("mm", 7, 0, 0),
)
BLOCKS = ((0, 0), (1, 0), (2, 0), (0, 1), (1, 1), (2, 1), (3, 0), (3, 1))
EARLY = (0, 1)
WAY = ((1, 1), (1, 0, 0))
SHIFT = (2, 1, 3, 0)
GROUPS = ((0, 1), (2, 3)), ((0, 1), (2,), (3,))


def kernel(q_hbm, k_hbm, v_hbm, g_hbm, ae_ref, ge_ref, out_ref,
           q_ref, k_ref, v_ref, g_in, vt_ref, g_send, g_all, at_own, at_oth,
           z2_send, z2_recv, zf_send, zf_recv, f_send, f_recv, p_send, p_recv, e_send, e_recv, s_send, s_recv, out_v,
           in_sem, s1_ssem, s1_rsem, x_ssem, x_rsem, xf_ssem, xf_rsem, a_ssem, a_rsem,
           z2_ssem, z2_rsem, zf_ssem, zf_rsem, f_ssem, f_rsem, l_ssem, l_rsem, out_sem):
    d = lax.axis_index("dp")
    t = lax.axis_index("tensor")
    yh, z, c = lax.div(d, 8), lax.rem(lax.div(d, 2), 4), lax.rem(d, 2)
    low, x = lax.div(t, 4), lax.rem(t, 4)
    half = lax.rem(low + yh, 2)
    partner_dp = d + 1 - 2 * c
    side_t = (1 - low) * 4 + x
    x_up, x_down, x_far = lax.rem(x + 1, 4), lax.rem(x + 3, 4), lax.rem(x + 2, 4)
    z_up, z_down = lax.rem(z + 1, 4), lax.rem(z + 3, 4)

    def dev(dp, tensor):
        return {"dp": dp, "tensor": tensor}

    core_dev, side_dev, cross_dev = dev(partner_dp, t), dev(d, side_t), dev(partner_dp, side_t)
    x_devs = dev(d, low * 4 + x_up), dev(d, low * 4 + x_down)
    z_devs = tuple(dev(yh * 8 + to * 2 + c, t) for to in (z_up, z_down, lax.rem(z + 2, 4)))
    far_dev = dev((1 - yh) * 8 + z * 2 + c, side_t)
    quarter_dev = (core_dev, side_dev, cross_dev)
    quarter_slot = ((1 - c, low), (c, 1 - low), (1 - c, 1 - low))

    def remote(src, dst, ssem, rsem, to):
        return pltpu.make_async_remote_copy(
            src_ref=src, dst_ref=dst, send_sem=ssem, recv_sem=rsem, device_id=to, device_id_type=MESH
        )

    def start(make, *key):
        make(*key).start()

    def sent(ref, ssem):
        remote(ref, ref, ssem, in_sem.at[0], core_dev).wait_send()

    loads = [
        pltpu.make_async_copy(src, dst, in_sem.at[i])
        for i, (src, dst) in enumerate(((g_hbm, g_in), (k_hbm, k_ref), (v_hbm, v_ref), (q_hbm, q_ref)))
    ]
    for load in loads:
        load.start()
    barrier = pltpu.get_barrier_semaphore()
    for to in (core_dev, side_dev, cross_dev, *x_devs, *z_devs, far_dev):
        pl.semaphore_signal(barrier, inc=1, device_id=to, device_id_type=MESH)

    grad_factor = SATURATION * jnp.exp2(jnp.full((1, 256), -ge_ref[0], jnp.int32).astype(F32))
    act_factor = SATURATION * jnp.exp2(jnp.full((1, 256), -ae_ref[0], jnp.int32).astype(F32))
    dequant = jnp.exp2(jnp.full((1, 256), ae_ref[0] + ge_ref[0], jnp.int32).astype(F32)) / (
        SATURATION * SATURATION
    )

    loads[0].wait()

    def scaled(block):
        values = g_in[:, pl.ds(pl.multiple_of(block * 256, 256), 256)].astype(F32)
        return jnp.clip(values * grad_factor, -SATURATION, SATURATION).astype(BF16)

    for o, (role, near) in enumerate(BLOCKS):
        to_yh = yh if near else 1 - yh
        base = to_yh * 16 + lax.rem(z + SHIFT[role], 4) * 4
        g_send[1, o] = scaled(base + 2 * c + 1 - half)
        g_send[2, o] = scaled(base + 2 * (1 - c) + 1 - half)
        g_send[0, o] = scaled(base + 2 * (1 - c) + half)
        g_all[o, c, low, x] = scaled(base + 2 * c + half)
    pl.semaphore_wait(barrier, 9)

    def s1_copy(k, o):
        return remote(g_send.at[k, o], g_all.at[o, c, low, x], s1_ssem.at[0], s1_rsem.at[k, o], quarter_dev[k])

    def s1_wait(k, o):
        s, l = quarter_slot[k]
        remote(g_send.at[k, o], g_all.at[o, s, l, x], s1_ssem.at[0], s1_rsem.at[k, o], quarter_dev[k]).wait_recv()

    def x_copy(o, i, part, at):
        if part == 2:
            ref = g_all.at[o, :, 1 - low, at]
        else:
            ref = g_all.at[o, 1 - c if part else c, low, at]
        return remote(ref, ref, x_ssem.at[i], x_rsem.at[i, o], x_devs[i])

    def xf_copy(o, i, at):
        ref = g_all.at[o, i, :, at]
        return remote(ref, ref, xf_ssem.at[i], xf_rsem.at[i, o], x_devs[i])

    def a_copy(i, q):
        rows = pl.ds(q * 256, 256)
        src = (at_oth if i == 2 else at_own).at[c, rows]
        dst = (at_own if i == 0 else at_oth).at[c, rows]
        return remote(src, dst, a_ssem.at[i], a_rsem.at[i, q], (core_dev, side_dev, core_dev)[i])

    def a_wait(i, q):
        rows = pl.ds(q * 256, 256)
        ref = (at_own if i == 0 else at_oth).at[c if i == 1 else 1 - c, rows]
        remote(ref, ref, a_ssem.at[i], a_rsem.at[i, q], (core_dev, side_dev, core_dev)[i]).wait_recv()

    have = set()

    def need(key, wait):
        if key not in have:
            have.add(key)
            wait()

    def need_x(o, i):
        ref = g_all.at[o, :, :, (x_down, x_up)[i]]
        need(("x", o, i), lambda: remote(ref, ref, x_ssem.at[i], x_rsem.at[i, o], x_devs[i]).wait_recv())

    def head(index):
        columns = slice(index * HEAD_DIM, (index + 1) * HEAD_DIM)
        for tb in range(4):
            rows = slice(tb * 256, (tb + 1) * 256)
            query = q_ref[rows, columns]

            def scores_of(keys):
                return lax.dot_general(keys, query, (((1,), (1,)), ((), ())), preferred_element_type=F32)

            last = jnp.where(causal, scores_of(k_ref[rows, :]), F32(-1e30))
            top = jnp.max(last, axis=0, keepdims=True)
            if tb > 0:
                early = scores_of(k_ref[: tb * 256, :])
                top = jnp.maximum(top, jnp.max(early, axis=0, keepdims=True))
            weights = jnp.exp2((last - top) * EXPONENT_SCALE)
            total = jnp.sum(weights, axis=0, keepdims=True)
            value = jnp.dot(vt_ref[:, rows], weights.astype(BF16), preferred_element_type=F32)
            if tb > 0:
                weights = jnp.exp2((early - top) * EXPONENT_SCALE)
                total += jnp.sum(weights, axis=0, keepdims=True)
                value += jnp.dot(vt_ref[:, : tb * 256], weights.astype(BF16), preferred_element_type=F32)
            value = jnp.clip(value * (act_factor / total), -SATURATION, SATURATION).astype(BF16)
            at_own[c, columns, rows] = value

    def z2_copy(stream, way, q):
        return remote(z2_send.at[stream, q], z2_recv.at[stream, q], z2_ssem.at[stream // 2], z2_rsem.at[stream, q],
                      z_devs[way])

    def zf_copy(way, stream, q):
        return remote(zf_send.at[way, stream, q], zf_recv.at[way, stream, q], zf_ssem.at[stream // 2],
                      zf_rsem.at[way, stream, q], z_devs[way])

    def f_copy(role, to_which, q):
        at = role, to_which, q - EARLY[0]
        return remote(f_send.at[at], f_recv.at[at], f_ssem.at[0], f_rsem.at[at], far_dev)

    def last_copy(i, q):
        send, recv = (p_send, e_send, s_send)[i], (p_recv, e_recv, s_recv)[i]
        return remote(send.at[q], recv.at[q], l_ssem.at[i], l_rsem.at[i, q], (far_dev, far_dev, side_dev)[i])

    def out_copy(part, q):
        side = 1 - half if part else half
        to = out_ref.at[pl.ds(q * 256, 256), pl.ds(pl.multiple_of(side * 256, 256), 256)]
        return pltpu.make_async_copy(out_v.at[part, q], to, out_sem.at[part, q])

    def multiply(o, which, group):
        role, near = BLOCKS[o]
        quarters = GROUPS[which][group]
        stream, way2 = 2 * near + which, WAY[which][group]
        early = quarters[0] in EARLY
        for part in range(3):
            need(("s1", o, part), None)
        for i in range(2):
            need_x(o, i)
            need(("xf", o, i), lambda: xf_copy(o, i, x_far).wait_recv())
        adds, make, key, send = [], None, (), None
        for q in quarters:
            need(("cols", q) if which == OWN else ("relay", q), None)
            need(("a", which, q), lambda: a_wait(2 * which, q))
        if early and not near:
            make, key, send = f_copy, (role, 1 - which), lambda q: f_send.at[role, 1 - which, q - EARLY[0]]
        else:
            if early:
                for q in quarters:
                    f_copy(role, which, q).wait_recv()
                adds.append(lambda q: f_recv.at[role, which, q - EARLY[0]])
            if role == 0:
                make, key, send = z2_copy, (stream, way2), lambda q: z2_send.at[stream, q]
            elif role < 3:
                make, key, send = zf_copy, (role - 1, stream), lambda q: zf_send.at[role - 1, stream, q]
                if role - 1 == way2:
                    for q in quarters:
                        z2_copy(stream, way2, q).wait_recv()
                    adds.append(lambda q: z2_recv.at[stream, q])
            else:
                for q in quarters:
                    for way in range(2):
                        zf_copy(way, stream, q).wait_recv()
                adds += [lambda q: zf_recv.at[0, stream, q], lambda q: zf_recv.at[1, stream, q]]
                if way2 == 2:
                    for q in quarters:
                        z2_copy(stream, way2, q).wait_recv()
                    adds.append(lambda q: z2_recv.at[stream, q])
                if not near:
                    make, key, send = last_copy, (which,), lambda q: (p_send, e_send)[which].at[q]
                elif which == OTHER:
                    make, key, send = last_copy, (2,), lambda q: s_send.at[q]
                    if not early:
                        for q in quarters:
                            last_copy(0, q).wait_recv()
                        adds.append(lambda q: p_recv.at[q])
        at = (at_own, at_oth)[which]

        def tile(q):
            rows = pl.ds(q * 256 if isinstance(q, int) else pl.multiple_of(q * 256, 256), 256)
            total = jnp.dot(at[0, rows, :], g_all[o, 0].reshape(1024, 256), preferred_element_type=F32)
            total += jnp.dot(at[1, rows, :], g_all[o, 1].reshape(1024, 256), preferred_element_type=F32)
            for add in adds:
                total += add(q)[...].astype(F32)
            if make is None:
                out_v[0, q] = total * dequant
                if early:
                    out_copy(0, q).start()
            else:
                send(q)[...] = total.astype(BF16)
                make(*key, q).start()

        if len(quarters) == 1:
            tile(quarters[0])
        else:
            lax.fori_loop(0, len(quarters), lambda i, carry: (tile(quarters[0] + i), carry)[1], 0)

    for o in range(8):
        start(s1_copy, 0, o)
    causal = None
    for step in STEPS:
        kind, at = step[0], step[1]
        if kind == "rows":
            start(s1_copy, 1, at)
            start(s1_copy, 2, at)
        elif kind == "self":
            have.add(("s1", at, 0))
            for i in range(2):
                start(x_copy, at, i, 0, x)
        elif kind == "near":
            s1_wait(0, at)
            have.add(("s1", at, 1))
            for i in range(2):
                start(x_copy, at, i, 1, x)
        elif kind == "side":
            s1_wait(1, at)
            s1_wait(2, at)
            have.add(("s1", at, 2))
            for i in range(2):
                start(x_copy, at, i, 2, x)
        elif kind == "pass":
            for i in range(2):
                need_x(at, i)
                start(xf_copy, at, i, (x_down, x_up)[i])
        elif kind == "head":
            if at == 0:
                for load in loads[1:]:
                    load.wait()
                vt_ref[...] = v_ref[...].astype(F32).T.astype(BF16)
                causal = lax.broadcasted_iota(jnp.int32, (256, 256), 0) <= lax.broadcasted_iota(
                    jnp.int32, (256, 256), 1
                )
            head(at)
        elif kind == "cols":
            have.add(("cols", at))
            start(a_copy, 0, at)
            start(a_copy, 1, at)
        elif kind == "relay":
            a_wait(1, at)
            have.add(("relay", at))
            start(a_copy, 2, at)
        else:
            multiply(*step[1:])

    for q in range(4):
        if q not in EARLY:
            last_copy(1, q).wait_recv()
            out_v[0, q] += e_recv[q].astype(F32) * dequant
            out_copy(0, q).start()
    for q in range(4):
        last_copy(2, q).wait_recv()
        out_v[1, q] = s_recv[q].astype(F32) * dequant
        out_copy(1, q).start()
    late = slice(0, 4)
    if EARLY:
        late = slice(2, 4) if EARLY[0] == 0 else slice(0, 2)
        sent(f_send, f_ssem.at[0])
    sent(g_send, s1_ssem.at[0])
    for i in range(2):
        sent(g_all.at[:, :, :, x], x_ssem.at[i])
        sent(g_all.at[:, i, :, (x_down, x_up)[i]], xf_ssem.at[i])
        sent((p_send, e_send)[i].at[late], l_ssem.at[i])
    for i, ref in enumerate((at_own, at_own, at_oth)):
        sent(ref.at[c], a_ssem.at[i])
    sent(z2_send.at[2:4], z2_ssem.at[1])
    sent(z2_send.at[0:2, late], z2_ssem.at[0])
    sent(zf_send.at[:, 2:4], zf_ssem.at[1])
    sent(zf_send.at[:, 0:2, late], zf_ssem.at[0])
    sent(s_send, l_ssem.at[2])
    for q in range(4):
        for part in range(2):
            out_copy(part, q).wait()


def on_device(queries, keys, values, out_grad, act_exponent, grad_exponent):
    anywhere = pl.BlockSpec(memory_space=pl.ANY)
    scalar = pl.BlockSpec(memory_space=pltpu.SMEM)
    dma = pltpu.SemaphoreType.DMA
    early = max(len(EARLY), 1)
    tile = (256, 256)
    transposed = pl.pallas_call(
        kernel,
        name="project_grad",
        out_shape=jax.ShapeDtypeStruct((1024, 512), F32),
        in_specs=[anywhere] * 4 + [scalar] * 2,
        out_specs=anywhere,
        scratch_shapes=[
            pltpu.VMEM((1024, 1024), BF16),
            pltpu.VMEM((1024, 128), BF16),
            pltpu.VMEM((1024, 128), BF16),
            pltpu.VMEM((128, 8192), BF16),
            pltpu.VMEM((128, 1024), BF16),
            pltpu.VMEM((3, 8, 128, 256), BF16),
            pltpu.VMEM((8, 2, 2, 4, 128, 256), BF16),
            pltpu.VMEM((2, 1024, 1024), BF16),
            pltpu.VMEM((2, 1024, 1024), BF16),
            pltpu.VMEM((4, 4, *tile), BF16), pltpu.VMEM((4, 4, *tile), BF16),
            pltpu.VMEM((2, 4, 4, *tile), BF16), pltpu.VMEM((2, 4, 4, *tile), BF16),
            pltpu.VMEM((4, 2, early, *tile), BF16), pltpu.VMEM((4, 2, early, *tile), BF16),
            pltpu.VMEM((4, *tile), BF16), pltpu.VMEM((4, *tile), BF16),
            pltpu.VMEM((4, *tile), BF16), pltpu.VMEM((4, *tile), BF16),
            pltpu.VMEM((4, *tile), BF16), pltpu.VMEM((4, *tile), BF16),
            pltpu.VMEM((2, 4, *tile), F32),
            dma((4,)),
            dma((1,)), dma((3, 8)),
            dma((2,)), dma((2, 8)),
            dma((2,)), dma((2, 8)),
            dma((3,)), dma((3, 4)),
            dma((2,)), dma((4, 4)),
            dma((2,)), dma((2, 4, 4)),
            dma((1,)), dma((4, 2, early)),
            dma((3,)), dma((3, 4)),
            dma((2, 4)),
        ],
        compiler_params=pltpu.CompilerParams(
            collective_id=0, has_side_effects=True, vmem_limit_bytes=VMEM_LIMIT
        ),
    )(queries, keys, values, out_grad, act_exponent, grad_exponent)
    return transposed.T


def solution(mesh):
    in_specs = (
        P("dp", "tensor"),
        P("dp", "tensor"),
        P("dp", "tensor"),
        P(("dp", "tensor"), None),
        P(),
        P(),
    )
    return jax.shard_map(
        on_device, mesh=mesh, in_specs=in_specs, out_specs=P("dp", "tensor"), check_vma=False
    )
```
